32 devices in a mesh: zero: 8 (over y, x, core), width: 4 (over z).
Axes of the slice: x: 2, y: 2, z: 4, core: 2. Of those that a mesh axis runs over, the one named last changes fastest.
Arguments:
- train_query: bfloat16 [4608, 4096], P('zero', 'width'), may hold values from -0.09375 to 0.09375
- low_query: bfloat16 [4608, 64], P('zero'), may hold values from -0.09375 to 0.09375
- high_query: bfloat16 [64, 4096], P(None, 'width'), may hold values from -0.75 to 0.75
- train_key: bfloat16 [4608, 2048], P('zero', 'width'), may hold values from -0.09375 to 0.09375
- low_key: bfloat16 [4608, 64], P('zero'), may hold values from -0.09375 to 0.09375
- high_key: bfloat16 [64, 2048], P(None, 'width'), may hold values from -0.75 to 0.75
- train_value: bfloat16 [4608, 2048], P('zero', 'width'), may hold values from -0.09375 to 0.09375
- low_value: bfloat16 [4608, 64], P('zero'), may hold values from -0.09375 to 0.09375
- high_value: bfloat16 [64, 2048], P(None, 'width'), may hold values from -0.75 to 0.75
- train_mixed: bfloat16 [4096, 4608], P('width', 'zero'), may hold values from -0.09375 to 0.09375
- low_mixed: bfloat16 [4096, 64], P('width'), may hold values from -0.09375 to 0.09375
- high_mixed: bfloat16 [64, 4608], P(None, 'zero'), may hold values from -0.75 to 0.75
- norm_train: float32 [4608], P(('zero', 'width')), may hold values from 0.25 to 1.75
- norm_step: float32 [4608], P(('zero', 'width')), may hold values from -0.3 to 0.3
Outputs:
- final_query: bfloat16 [4608, 4096], P(None, 'width')
- final_key: bfloat16 [4608, 2048], P(None, 'width')
- final_value: bfloat16 [4608, 2048], P(None, 'width')
- final_mixed: bfloat16 [4096, 4608], P('width')
- serve_norm: bfloat16 [4608], replicated
The draws below stay inside these ranges and needn't reach their ends.
All inputs are finite; a program needn't handle non-finite values.
Results may differ from the reference program's by a relative error of at most 0.001.
Values may be sent and summed in bfloat16 or wider, within the bound.
No kernel may reach another device: no remote copies, remote signals or barrier semaphores. Data moves between devices by JAX's collectives and lax.ppermute only.
A program may use at most 192 MiB of HBM per device.

```python
import jax
import jax.numpy as jnp

D_MODEL = 4608
Q_DIM = 4096
KV_DIM = 2048
RANK = 64


def levels(stream_key, dims, pieces, low, largest):
    def one(position, parts):
        draws = jax.random.uniform(jax.random.fold_in(jax.random.fold_in(stream_key, 6), position), (parts,), jnp.float32, low / len(pieces), largest / len(pieces))
        return jnp.repeat(jnp.exp(draws), dims[position] // parts).reshape((-1,) + (1,) * (len(dims) - position - 1))

    loudness = one(*pieces[0])
    for cut in pieces[1:]:
        loudness = loudness * one(*cut)
    return loudness


def gaussian(key, shape, scale, bound, pieces=(), held_as=jnp.bfloat16):
    result = jax.random.normal(key, shape, jnp.float32) * scale
    if len(pieces) > 0:
        result = levels(key, shape, pieces, -0.22, 0.18) * result
    return jnp.clip(result, min=-bound, max=bound).astype(held_as)


def setup_inputs(seed: int = 0) -> dict:
    key_of = jax.random.split(jax.random.key(seed), 15)
    train_query = gaussian(key_of[0], (D_MODEL, Q_DIM), D_MODEL ** -0.5, 0.09375, ((0, 8), (1, 4)))
    low_query = gaussian(key_of[1], (D_MODEL, RANK), D_MODEL ** -0.5, 0.09375, ((0, 8),))
    high_query = gaussian(key_of[2], (RANK, Q_DIM), RANK ** -0.5, 0.75, ((1, 4),))
    train_key = gaussian(key_of[3], (D_MODEL, KV_DIM), D_MODEL ** -0.5, 0.09375, ((0, 8), (1, 4)))
    low_key = gaussian(key_of[4], (D_MODEL, RANK), D_MODEL ** -0.5, 0.09375, ((0, 8),))
    high_key = gaussian(key_of[5], (RANK, KV_DIM), RANK ** -0.5, 0.75, ((1, 4),))
    train_value = gaussian(key_of[6], (D_MODEL, KV_DIM), D_MODEL ** -0.5, 0.09375, ((0, 8), (1, 4)))
    low_value = gaussian(key_of[7], (D_MODEL, RANK), D_MODEL ** -0.5, 0.09375, ((0, 8),))
    high_value = gaussian(key_of[8], (RANK, KV_DIM), RANK ** -0.5, 0.75, ((1, 4),))
    train_mixed = gaussian(key_of[9], (Q_DIM, D_MODEL), Q_DIM ** -0.5, 0.09375, ((0, 4), (1, 8)))
    low_mixed = gaussian(key_of[10], (Q_DIM, RANK), Q_DIM ** -0.5, 0.09375, ((0, 4),))
    high_mixed = gaussian(key_of[11], (RANK, D_MODEL), RANK ** -0.5, 0.75, ((1, 8),))
    norm_train = jnp.clip(1.0 + 0.15 * jax.random.normal(key_of[12], (D_MODEL,), jnp.float32), 0.25, 1.75)
    norm_step = jnp.clip(jax.random.uniform(key_of[13], (D_MODEL,), jnp.float32, -0.3, 0.3) * levels(key_of[13], (D_MODEL,), ((0, 32),), -0.4, 0.0), -0.3, 0.3)
    return {"train_query": train_query, "low_query": low_query, "high_query": high_query, "train_key": train_key, "low_key": low_key, "high_key": high_key, "train_value": train_value, "low_value": low_value, "high_value": high_value, "train_mixed": train_mixed, "low_mixed": low_mixed, "high_mixed": high_mixed, "norm_train": norm_train, "norm_step": norm_step}


mix_rate = 0.5


def reference(train_query, low_query, high_query, train_key, low_key, high_key, train_value, low_value, high_value, train_mixed, low_mixed, high_mixed, norm_train, norm_step):
    result_query = train_query.astype(jnp.float32) + mix_rate * jnp.dot(low_query, high_query, preferred_element_type=jnp.float32)
    result_key = train_key.astype(jnp.float32) + mix_rate * jnp.dot(low_key, high_key, preferred_element_type=jnp.float32)
    result_value = train_value.astype(jnp.float32) + mix_rate * jnp.dot(low_value, high_value, preferred_element_type=jnp.float32)
    result_mixed = train_mixed.astype(jnp.float32) + mix_rate * jnp.dot(low_mixed, high_mixed, preferred_element_type=jnp.float32)
    final_query = result_query.astype(jnp.bfloat16)
    final_key = result_key.astype(jnp.bfloat16)
    final_value = result_value.astype(jnp.bfloat16)
    final_mixed = result_mixed.astype(jnp.bfloat16)
    serve_norm = (norm_train + norm_step).astype(jnp.bfloat16)
    return final_query, final_key, final_value, final_mixed, serve_norm
```

```python
import math

import jax
import jax.numpy as jnp
from jax import lax
from jax.experimental import pallas as pl
from jax.experimental.pallas import tpu as pltpu
from jax.sharding import PartitionSpec as P

mix_rate = 0.5


def merged(train, low, high):
    update = jnp.dot(low, high, preferred_element_type=jnp.float32)
    return (train.astype(jnp.float32) + mix_rate * update).astype(jnp.bfloat16)


def place(targets, moves, offsets, shapes):
    pieces = [move[0] for move in moves]
    count = len(pieces)
    kept = [index for index, target in enumerate(targets) if target is not None]

    def body(offsets_ref, *refs):
        sources = refs[:count]
        outputs = refs[count + len(kept) : count + len(kept) + len(shapes)]
        semaphores = refs[-1]
        copies = []
        for index, (piece, output, row, column) in enumerate(moves):
            rows = pl.ds(pl.multiple_of(offsets_ref[row], 16), piece.shape[0])
            columns = pl.ds(pl.multiple_of(offsets_ref[column], 128), piece.shape[1])
            copy = pltpu.make_async_copy(
                sources[index], outputs[output].at[rows, columns], semaphores.at[index]
            )
            copy.start()
            copies.append(copy)
        for copy in copies:
            copy.wait()

    anywhere = pl.BlockSpec(memory_space=pl.ANY)
    return pl.pallas_call(
        body,
        out_shape=[jax.ShapeDtypeStruct(shape, jnp.bfloat16) for shape in shapes],
        in_specs=[pl.BlockSpec(memory_space=pltpu.SMEM)] + [anywhere] * (count + len(kept)),
        out_specs=[anywhere] * len(shapes),
        scratch_shapes=[pltpu.SemaphoreType.DMA((count,))],
        input_output_aliases={1 + count + place_: index for place_, index in enumerate(kept)},
    )(offsets, *pieces, *[targets[index] for index in kept])


def solution(mesh):
    zero, width = mesh.shape["zero"], mesh.shape["width"]
    cores = 2 if zero % 2 == 0 else 1
    chips = zero // cores
    side_y = max(n for n in range(1, math.isqrt(chips) + 1) if chips % n == 0)
    side_x = chips // side_y

    def number(y, x, core):
        return ((y % side_y) * side_x + x % side_x) * cores + core % cores

    def shift(value, dy=0, dx=0, dcore=0):
        pairs = [
            (number(y + dy, x + dx, core + dcore), number(y, x, core))
            for y in range(side_y)
            for x in range(side_x)
            for core in range(cores)
        ]
        return lax.ppermute(value, "zero", pairs)

    def gather_norm(norm, y, x, core):
        around = [norm]
        for step in range(1, width):
            pairs = [((z + step) % width, z) for z in range(width)]
            around.append(lax.ppermute(norm, "width", pairs))
        gathered = jnp.roll(jnp.stack(around), lax.axis_index("width"), axis=0)
        for size, place_, move in (
            (cores, core, {"dcore": 1}),
            (side_x, x, {"dx": 1}),
            (side_y, y, {"dy": 1}),
        ):
            around = [gathered]
            for _ in range(size - 1):
                around.append(shift(around[-1], **move))
            gathered = jnp.roll(jnp.stack(around), place_, axis=0)
        return gathered.reshape(-1)

    def on_device(
        train_query,
        low_query,
        high_query,
        train_key,
        low_key,
        high_key,
        train_value,
        low_value,
        high_value,
        train_mixed,
        low_mixed,
        high_mixed,
        norm_train,
        norm_step,
    ):
        norm = (norm_train + norm_step).astype(jnp.bfloat16)
        key = merged(train_key, low_key, high_key)
        mixed = merged(train_mixed, low_mixed, high_mixed)
        value = merged(train_value, low_value, high_value)
        query = merged(train_query, low_query, high_query)
        rows, columns = query.shape[0], mixed.shape[1]
        aligned = rows % 16 == 0 and (cores * columns) % 128 == 0
        aligned = aligned and mixed.shape[0] % (16 * cores) == 0
        if not aligned or cores == 1:
            return (
                lax.all_gather(query, "zero", axis=0, tiled=True),
                lax.all_gather(key, "zero", axis=0, tiled=True),
                lax.all_gather(value, "zero", axis=0, tiled=True),
                lax.all_gather(mixed, "zero", axis=1, tiled=True),
                lax.all_gather(norm, ("zero", "width"), axis=0, tiled=True),
            )

        index = lax.axis_index("zero")
        core = index % cores
        x = (index // cores) % side_x
        y = index // (cores * side_x)

        other_mixed = shift(mixed, dcore=1)
        pair = jnp.where(
            core == 0,
            jnp.concatenate([mixed, other_mixed], axis=1),
            jnp.concatenate([other_mixed, mixed], axis=1),
        )
        half = mixed.shape[0] // cores
        mixed_part = lax.dynamic_slice_in_dim(pair, core * half, half, axis=0)

        def x_first(own):
            held = {(0, 0): own}
            for dx in range(1, side_x):
                held[0, dx] = shift(held[0, dx - 1], dx=1)
            for dy in range(1, side_y):
                for dx in range(side_x):
                    held[dy, dx] = shift(held[dy - 1, dx], dy=1)
            return held

        def y_first(own):
            held = {(0, 0): own}
            for dy in range(1, side_y):
                held[dy, 0] = shift(held[dy - 1, 0], dy=1)
            for dx in range(1, side_x):
                for dy in range(side_y):
                    held[dy, dx] = shift(held[dy, dx - 1], dx=1)
            return held

        keys, queries = x_first(key), x_first(query)
        values, mixeds = y_first(value), y_first(mixed_part)

        offsets = [jnp.zeros_like(index), core * half, (1 - core) * half]
        slots = {}
        for dy in range(side_y):
            for dx in range(side_x):
                chip = ((y + dy) % side_y) * side_x + (x + dx) % side_x
                slots[dy, dx] = len(offsets)
                offsets += [
                    (chip * cores + core) * rows,
                    (chip * cores + 1 - core) * rows,
                    chip * (cores * columns),
                ]
        offsets = jnp.stack(offsets).astype(jnp.int32)

        def moves_of(held, output, spot):
            piece, slot = held[spot], slots[spot]
            if output == 3:
                if spot == (0, 0):
                    return [(pair, 3, 0, slot + 2)]
                return [
                    (piece, 3, 1, slot + 2),
                    (shift(piece, dcore=1), 3, 2, slot + 2),
                ]
            return [
                (piece, output, slot, 0),
                (shift(piece, dcore=1), output, slot + 1, 0),
            ]

        shapes = [
            (rows * zero, query.shape[1]),
            (rows * zero, key.shape[1]),
            (rows * zero, value.shape[1]),
            (mixed.shape[0], columns * zero),
        ]
        corner = (side_y - 1, side_x - 1)
        first, second, third = [], [], []
        for output, held in ((0, queries), (1, keys), (2, values), (3, mixeds)):
            for spot in held:
                group = second
                if spot == (0, 0):
                    group = first
                elif spot == corner:
                    group = third
                group += moves_of(held, output, spot)
        outputs = [None] * 4
        for group in (first, second, third):
            if group:
                outputs = place(outputs, group, offsets, shapes)
        return (*outputs, gather_norm(norm, y, x, core))

    return jax.shard_map(
        on_device,
        mesh=mesh,
        in_specs=(
            P("zero", "width"),
            P("zero", None),
            P(None, "width"),
            P("zero", "width"),
            P("zero", None),
            P(None, "width"),
            P("zero", "width"),
            P("zero", None),
            P(None, "width"),
            P("width", "zero"),
            P("width", None),
            P(None, "zero"),
            P(("zero", "width")),
            P(("zero", "width")),
        ),
        out_specs=(P(None, "width"), P(None, "width"), P(None, "width"), P("width", None), P()),
        check_vma=False,
    )
```

```python
import math

import jax
import jax.numpy as jnp
from jax import lax
from jax.experimental import pallas as pl
from jax.experimental.pallas import tpu as pltpu
from jax.sharding import PartitionSpec as P


mix_rate = 0.5


def merged(train, low, high):
    update = jnp.dot(low, high, preferred_element_type=jnp.float32)
    return (train.astype(jnp.float32) + mix_rate * update).astype(jnp.bfloat16)


def place(targets, moves, offsets, shapes):
    pieces = [move[0] for move in moves]
    count = len(pieces)
    kept = [index for index, target in enumerate(targets) if target is not None]

    def body(offsets_ref, *refs):
        sources = refs[:count]
        outputs = refs[count + len(kept) : count + len(kept) + len(shapes)]
        stages = refs[-count - 2 : -2]
        arrivals, departures = refs[-2:]
        loads, stores = [], []
        for index, (piece, output, row, column) in enumerate(moves):
            rows = pl.ds(pl.multiple_of(offsets_ref[row], 16), piece.shape[0])
            columns = pl.ds(pl.multiple_of(offsets_ref[column], 128), piece.shape[1])
            loads.append(
                pltpu.make_async_copy(sources[index], stages[index], arrivals.at[index])
            )
            stores.append(
                pltpu.make_async_copy(
                    stages[index], outputs[output].at[rows, columns], departures.at[index]
                )
            )
        for load in loads:
            load.start()
        for load, store in zip(loads, stores):
            load.wait()
            store.start()
        for store in stores:
            store.wait()

    anywhere = pl.BlockSpec(memory_space=pl.ANY)
    return pl.pallas_call(
        body,
        out_shape=[jax.ShapeDtypeStruct(shape, jnp.bfloat16) for shape in shapes],
        in_specs=[pl.BlockSpec(memory_space=pltpu.SMEM)] + [anywhere] * (count + len(kept)),
        out_specs=[anywhere] * len(shapes),
        scratch_shapes=[pltpu.VMEM(piece.shape, piece.dtype) for piece in pieces]
        + [pltpu.SemaphoreType.DMA((count,)), pltpu.SemaphoreType.DMA((count,))],
        input_output_aliases={1 + count + place_: index for place_, index in enumerate(kept)},
        compiler_params=pltpu.CompilerParams(vmem_limit_bytes=40 * 2**20),
    )(offsets, *pieces, *[targets[index] for index in kept])


def solution(mesh):
    zero, width = mesh.shape["zero"], mesh.shape["width"]
    cores = 2 if zero % 2 == 0 else 1
    chips = zero // cores
    side_y = max(n for n in range(1, math.isqrt(chips) + 1) if chips % n == 0)
    side_x = chips // side_y

    def number(y, x, core):
        return ((y % side_y) * side_x + x % side_x) * cores + core % cores

    def shift(value, dy=0, dx=0, dcore=0):
        pairs = [
            (number(y + dy, x + dx, core + dcore), number(y, x, core))
            for y in range(side_y)
            for x in range(side_x)
            for core in range(cores)
        ]
        return lax.ppermute(value, "zero", pairs)

    def gather_norm(norm, y, x, core):
        around = [norm]
        for step in range(1, width):
            pairs = [((z + step) % width, z) for z in range(width)]
            around.append(lax.ppermute(norm, "width", pairs))
        gathered = jnp.roll(jnp.stack(around), lax.axis_index("width"), axis=0)
        around = [gathered]
        for step in range(1, cores):
            around.append(shift(gathered, dcore=step))
        gathered = jnp.roll(jnp.stack(around), core, axis=0)
        around = []
        for dy in range(side_y):
            for dx in range(side_x):
                if dy == 0 and dx == 0:
                    around.append(gathered)
                else:
                    around.append(shift(gathered, dy=dy, dx=dx))
        around = jnp.stack(around).reshape(side_y, side_x, -1)
        return jnp.roll(around, (y, x), axis=(0, 1)).reshape(-1)

    corner = (side_y - 1, side_x - 1)
    spots = [(dy, dx) for dy in range(side_y) for dx in range(side_x)]
    groups = [
        [(output, (0, 0)) for output in range(4)]
        + [(output, spot) for output in (0, 1) for spot in spots if spot[0] == 0 and spot[1] > 0]
        + [(output, spot) for output in (2, 3) for spot in spots if spot[1] == 0 and spot[0] > 0],
    ]
    rest = [(output, spot) for output in range(4) for spot in spots if (output, spot) not in groups[0]]
    groups += [
        [(output, spot) for output, spot in rest if spot != corner],
        [(output, spot) for output, spot in rest if spot == corner and output in (0, 3)],
        [(output, spot) for output, spot in rest if spot == corner and output in (1, 2)],
    ]

    def on_device(
        train_query,
        low_query,
        high_query,
        train_key,
        low_key,
        high_key,
        train_value,
        low_value,
        high_value,
        train_mixed,
        low_mixed,
        high_mixed,
        norm_train,
        norm_step,
    ):
        norm = (norm_train + norm_step).astype(jnp.bfloat16)
        key = merged(train_key, low_key, high_key)
        mixed = merged(train_mixed, low_mixed, high_mixed)
        value = merged(train_value, low_value, high_value)
        query = merged(train_query, low_query, high_query)
        rows, columns = query.shape[0], mixed.shape[1]
        aligned = rows % 16 == 0 and (cores * columns) % 128 == 0
        aligned = aligned and mixed.shape[0] % (16 * cores) == 0
        if not aligned or cores == 1:
            return (
                lax.all_gather(query, "zero", axis=0, tiled=True),
                lax.all_gather(key, "zero", axis=0, tiled=True),
                lax.all_gather(value, "zero", axis=0, tiled=True),
                lax.all_gather(mixed, "zero", axis=1, tiled=True),
                lax.all_gather(norm, ("zero", "width"), axis=0, tiled=True),
            )

        index = lax.axis_index("zero")
        core = index % cores
        x = (index // cores) % side_x
        y = index // (cores * side_x)

        other_mixed = shift(mixed, dcore=1)
        pair = jnp.where(
            core == 0,
            jnp.concatenate([mixed, other_mixed], axis=1),
            jnp.concatenate([other_mixed, mixed], axis=1),
        )
        half = mixed.shape[0] // cores
        mixed_part = lax.dynamic_slice_in_dim(pair, core * half, half, axis=0)

        def x_first(own):
            held = {(0, 0): own}
            for dx in range(1, side_x):
                held[0, dx] = shift(held[0, dx - 1], dx=1)
            for dy in range(1, side_y):
                for dx in range(side_x):
                    held[dy, dx] = shift(held[dy - 1, dx], dy=1)
            return held

        def y_first(own):
            held = {(0, 0): own}
            for dy in range(1, side_y):
                held[dy, 0] = shift(held[dy - 1, 0], dy=1)
            for dx in range(1, side_x):
                for dy in range(side_y):
                    held[dy, dx] = shift(held[dy, dx - 1], dx=1)
            return held

        keys, queries = x_first(key), x_first(query)
        values, mixeds = y_first(value), y_first(mixed_part)

        offsets = [jnp.zeros_like(index), core * half, (1 - core) * half]
        slots = {}
        for dy in range(side_y):
            for dx in range(side_x):
                chip = ((y + dy) % side_y) * side_x + (x + dx) % side_x
                slots[dy, dx] = len(offsets)
                offsets += [
                    (chip * cores + core) * rows,
                    (chip * cores + 1 - core) * rows,
                    chip * (cores * columns),
                ]
        offsets = jnp.stack(offsets).astype(jnp.int32)

        def moves_of(held, output, spot):
            piece, slot = held[spot], slots[spot]
            if output == 3:
                if spot == (0, 0):
                    return [(pair, 3, 0, slot + 2)]
                return [
                    (piece, 3, 1, slot + 2),
                    (shift(piece, dcore=1), 3, 2, slot + 2),
                ]
            return [
                (piece, output, slot, 0),
                (shift(piece, dcore=1), output, slot + 1, 0),
            ]

        shapes = [
            (rows * zero, query.shape[1]),
            (rows * zero, key.shape[1]),
            (rows * zero, value.shape[1]),
            (mixed.shape[0], columns * zero),
        ]
        held_of = (queries, keys, values, mixeds)
        outputs = [None] * 4
        for group in groups:
            moves = [move for output, spot in group for move in moves_of(held_of[output], output, spot)]
            outputs = place(outputs, moves, offsets, shapes)
        return (*outputs, gather_norm(norm, y, x, core))

    return jax.shard_map(
        on_device,
        mesh=mesh,
        in_specs=(
            P("zero", "width"),
            P("zero", None),
            P(None, "width"),
            P("zero", "width"),
            P("zero", None),
            P(None, "width"),
            P("zero", "width"),
            P("zero", None),
            P(None, "width"),
            P("width", "zero"),
            P("width", None),
            P(None, "zero"),
            P(("zero", "width")),
            P(("zero", "width")),
        ),
        out_specs=(P(None, "width"), P(None, "width"), P(None, "width"), P("width", None), P()),
        check_vma=False,
    )
```

```python
import math

import jax
import jax.numpy as jnp
from jax import lax
from jax.experimental import pallas as pl
from jax.experimental.pallas import tpu as pltpu
from jax.sharding import PartitionSpec as P


mix_rate = 0.5


def merged(train, low, high):
    update = jnp.dot(low, high, preferred_element_type=jnp.float32)
    return (train.astype(jnp.float32) + mix_rate * update).astype(jnp.bfloat16)


def place(targets, moves, offsets, shapes):
    pieces = [move[0] for move in moves]
    count = len(pieces)
    kept = [index for index, target in enumerate(targets) if target is not None]

    def body(offsets_ref, *refs):
        sources = refs[:count]
        outputs = refs[count + len(kept) : count + len(kept) + len(shapes)]
        stages = refs[-count - 2 : -2]
        arrivals, departures = refs[-2:]
        loads, stores = [], []
        for index, (piece, output, row, column) in enumerate(moves):
            rows = pl.ds(pl.multiple_of(offsets_ref[row], 16), piece.shape[0])
            columns = pl.ds(pl.multiple_of(offsets_ref[column], 128), piece.shape[1])
            loads.append(
                pltpu.make_async_copy(sources[index], stages[index], arrivals.at[index])
            )
            stores.append(
                pltpu.make_async_copy(
                    stages[index], outputs[output].at[rows, columns], departures.at[index]
                )
            )
        for load in loads:
            load.start()
        for load, store in zip(loads, stores):
            load.wait()
            store.start()
        for store in stores:
            store.wait()

    anywhere = pl.BlockSpec(memory_space=pl.ANY)
    return pl.pallas_call(
        body,
        out_shape=[jax.ShapeDtypeStruct(shape, jnp.bfloat16) for shape in shapes],
        in_specs=[pl.BlockSpec(memory_space=pltpu.SMEM)] + [anywhere] * (count + len(kept)),
        out_specs=[anywhere] * len(shapes),
        scratch_shapes=[pltpu.VMEM(piece.shape, piece.dtype) for piece in pieces]
        + [pltpu.SemaphoreType.DMA((count,)), pltpu.SemaphoreType.DMA((count,))],
        input_output_aliases={1 + count + place_: index for place_, index in enumerate(kept)},
        compiler_params=pltpu.CompilerParams(vmem_limit_bytes=40 * 2**20),
    )(offsets, *pieces, *[targets[index] for index in kept])


def solution(mesh):
    zero, width = mesh.shape["zero"], mesh.shape["width"]
    cores = 2 if zero % 2 == 0 else 1
    chips = zero // cores
    side_y = max(n for n in range(1, math.isqrt(chips) + 1) if chips % n == 0)
    side_x = chips // side_y

    def number(y, x, core):
        return ((y % side_y) * side_x + x % side_x) * cores + core % cores

    def shift(value, dy=0, dx=0, dcore=0):
        pairs = [
            (number(y + dy, x + dx, core + dcore), number(y, x, core))
            for y in range(side_y)
            for x in range(side_x)
            for core in range(cores)
        ]
        return lax.ppermute(value, "zero", pairs)

    def gather_norm(norm, y, x, core):
        around = [norm]
        for step in range(1, width):
            pairs = [((z + step) % width, z) for z in range(width)]
            around.append(lax.ppermute(norm, "width", pairs))
        gathered = jnp.roll(jnp.stack(around), lax.axis_index("width"), axis=0)
        around = [gathered]
        for step in range(1, cores):
            around.append(shift(gathered, dcore=step))
        gathered = jnp.roll(jnp.stack(around), core, axis=0)
        around = []
        for dy in range(side_y):
            for dx in range(side_x):
                if dy == 0 and dx == 0:
                    around.append(gathered)
                else:
                    around.append(shift(gathered, dy=dy, dx=dx))
        around = jnp.stack(around).reshape(side_y, side_x, -1)
        return jnp.roll(around, (y, x), axis=(0, 1)).reshape(-1)

    corner = (side_y - 1, side_x - 1)
    spots = [(dy, dx) for dy in range(side_y) for dx in range(side_x)]
    groups = [
        [(output, (0, 0)) for output in range(4)]
        + [(1, spot) for spot in spots if spot != (0, 0) and 0 in spot]
        + [(0, spot) for spot in spots if spot[0] == 0 and spot[1] > 0]
        + [(output, spot) for output in (2, 3) for spot in spots if spot[1] == 0 and spot[0] > 0],
    ]
    rest = [(output, spot) for output in range(4) for spot in spots if (output, spot) not in groups[0]]
    groups += [
        [(output, spot) for output, spot in rest if spot != corner],
        [(output, spot) for output, spot in rest if spot == corner and output in (0, 3)],
        [(output, spot) for output, spot in rest if spot == corner and output in (1, 2)],
    ]

    def on_device(
        train_query,
        low_query,
        high_query,
        train_key,
        low_key,
        high_key,
        train_value,
        low_value,
        high_value,
        train_mixed,
        low_mixed,
        high_mixed,
        norm_train,
        norm_step,
    ):
        norm = (norm_train + norm_step).astype(jnp.bfloat16)
        key = merged(train_key, low_key, high_key)
        value = merged(train_value, low_value, high_value)
        query = merged(train_query, low_query, high_query)
        mixed = merged(train_mixed, low_mixed, high_mixed)
        rows, columns = query.shape[0], mixed.shape[1]
        aligned = rows % 16 == 0 and (cores * columns) % 128 == 0
        aligned = aligned and mixed.shape[0] % (16 * cores) == 0
        if not aligned or cores == 1:
            return (
                lax.all_gather(query, "zero", axis=0, tiled=True),
                lax.all_gather(key, "zero", axis=0, tiled=True),
                lax.all_gather(value, "zero", axis=0, tiled=True),
                lax.all_gather(mixed, "zero", axis=1, tiled=True),
                lax.all_gather(norm, ("zero", "width"), axis=0, tiled=True),
            )

        index = lax.axis_index("zero")
        core = index % cores
        x = (index // cores) % side_x
        y = index // (cores * side_x)

        other_mixed = shift(mixed, dcore=1)
        pair = jnp.where(
            core == 0,
            jnp.concatenate([mixed, other_mixed], axis=1),
            jnp.concatenate([other_mixed, mixed], axis=1),
        )
        half = mixed.shape[0] // cores
        mixed_part = lax.dynamic_slice_in_dim(pair, core * half, half, axis=0)

        def x_first(own):
            held = {(0, 0): own}
            for dx in range(1, side_x):
                held[0, dx] = shift(held[0, dx - 1], dx=1)
            for dy in range(1, side_y):
                for dx in range(side_x):
                    held[dy, dx] = shift(held[dy - 1, dx], dy=1)
            return held

        def y_first(own):
            held = {(0, 0): own}
            for dy in range(1, side_y):
                held[dy, 0] = shift(held[dy - 1, 0], dy=1)
            for dx in range(1, side_x):
                for dy in range(side_y):
                    held[dy, dx] = shift(held[dy, dx - 1], dx=1)
            return held

        keys, queries = x_first(key), x_first(query)
        values, mixeds = y_first(value), y_first(mixed_part)

        offsets = [jnp.zeros_like(index), core * half, (1 - core) * half]
        slots = {}
        for dy in range(side_y):
            for dx in range(side_x):
                chip = ((y + dy) % side_y) * side_x + (x + dx) % side_x
                slots[dy, dx] = len(offsets)
                offsets += [
                    (chip * cores + core) * rows,
                    (chip * cores + 1 - core) * rows,
                    chip * (cores * columns),
                ]
        offsets = jnp.stack(offsets).astype(jnp.int32)

        def moves_of(held, output, spot):
            piece, slot = held[spot], slots[spot]
            if output == 3:
                if spot == (0, 0):
                    return [(pair, 3, 0, slot + 2)]
                return [
                    (piece, 3, 1, slot + 2),
                    (shift(piece, dcore=1), 3, 2, slot + 2),
                ]
            return [
                (piece, output, slot, 0),
                (shift(piece, dcore=1), output, slot + 1, 0),
            ]

        shapes = [
            (rows * zero, query.shape[1]),
            (rows * zero, key.shape[1]),
            (rows * zero, value.shape[1]),
            (mixed.shape[0], columns * zero),
        ]
        held_of = (queries, keys, values, mixeds)
        serving_norm = gather_norm(norm, y, x, core)
        outputs = [None] * 4
        for step, group in enumerate(groups):
            if step == 2:
                offsets, serving_norm = lax.optimization_barrier((offsets, serving_norm))
            moves = [move for output, spot in group for move in moves_of(held_of[output], output, spot)]
            outputs = place(outputs, moves, offsets, shapes)
        return (*outputs, serving_norm)

    return jax.shard_map(
        on_device,
        mesh=mesh,
        in_specs=(
            P("zero", "width"),
            P("zero", None),
            P(None, "width"),
            P("zero", "width"),
            P("zero", None),
            P(None, "width"),
            P("zero", "width"),
            P("zero", None),
            P(None, "width"),
            P("width", "zero"),
            P("width", None),
            P(None, "zero"),
            P(("zero", "width")),
            P(("zero", "width")),
        ),
        out_specs=(P(None, "width"), P(None, "width"), P(None, "width"), P("width", None), P()),
        check_vma=False,
    )
```
